32 devices in a mesh: sample: 2 (over x), sy: 4 (over y, core), sz: 4 (over z).
Axes of the slice: x: 2, y: 2, z: 4, core: 2. Of those that a mesh axis runs over, the one named last changes fastest.
Arguments:
- volume: bfloat16 [2, 32, 16, 32, 128], P('sample', None, 'sz', 'sy'), may hold values from -22.5 to 22.5
- amax_history: float32 [4, 16], replicated, may hold values from 0.48 to 2.5
- conv_first: bfloat16 [27, 32, 32], replicated, may hold values from -0.21875 to 0.21875
- conv_second: bfloat16 [27, 32, 32], replicated, may hold values from -0.21875 to 0.21875
- conv_third: bfloat16 [27, 64, 32], P(None, 'sy'), may hold values from -0.21875 to 0.21875
- conv_fourth: bfloat16 [27, 64, 64], P(None, 'sy'), may hold values from -0.15625 to 0.15625
- gain_fine: float32 [2, 32], replicated, may hold values from 0.5 to 1.5
- shift_fine: float32 [2, 32], replicated, may hold values from -0.5 to 0.5
- gain_coarse: float32 [2, 64], P(None, 'sy'), may hold values from 0.5 to 1.5
- shift_coarse: float32 [2, 64], P(None, 'sy'), may hold values from -0.5 to 0.5
Outputs:
- skip_features: bfloat16 [2, 32, 16, 32, 128], P('sample', None, 'sz', 'sy')
- coarse_features: bfloat16 [2, 64, 8, 1024], P('sample', 'sy', 'sz')
- amax_now: float32 [4], replicated
The draws below stay inside these ranges and needn't reach their ends.
All inputs are finite; a program needn't handle non-finite values.
Results may differ from the reference program's by a relative error of at most 0.012.
Values may be sent and summed in bfloat16 or wider, within the bound.
A program may use at most 128 MiB of HBM per device.

```python
import jax
import jax.numpy as jnp
from jax import lax

C1 = 32
C2 = 64
NX = 128
HIST = 16
LAYERS = 4
SAMPLES = 2
NY = 32
NZ = 16


def draw_volume(key, part):
    shape_all = (SAMPLES, C1, NZ, NY, NX)
    sample_pos = lax.broadcasted_iota(jnp.float32, shape_all, 0) / max(SAMPLES - 1, 1)
    z_pos = lax.broadcasted_iota(jnp.float32, shape_all, 2) / NZ
    y_pos = lax.broadcasted_iota(jnp.float32, shape_all, 3) / NY
    scaling = (0.6 + 1.2 * sample_pos) * (0.5 + z_pos + y_pos)
    noise_part = jnp.clip(jax.random.normal(key, shape_all, jnp.float32), -5.0, 5.0)
    return (noise_part * scaling).astype(jnp.bfloat16)


def draw_amax_history(key, part):
    level_key = jax.random.fold_in(key, 11)
    entry_key = jax.random.fold_in(key, 12)
    level_log = jax.random.uniform(level_key, (LAYERS, 1), jnp.float32, jnp.log(0.8), jnp.log(2.5))
    entries = jax.random.uniform(entry_key, (LAYERS, HIST), jnp.float32, 0.6, 1.0)
    return jnp.exp(level_log) * entries


def level_of(stream_key, dims, cuts, least, largest):
    def one(position, shards_of):
        steps = jax.random.uniform(jax.random.fold_in(jax.random.fold_in(stream_key, 6), position), (shards_of,), jnp.float32, least / len(cuts), largest / len(cuts))
        return jnp.repeat(jnp.exp(steps), dims[position] // shards_of).reshape((-1,) + (1,) * (len(dims) - position - 1))

    factor_of = one(*cuts[0])
    for cut in cuts[1:]:
        factor_of = factor_of * one(*cut)
    return factor_of


def gaussian(own_key, shape, scale, most, cuts=(), held_as=jnp.bfloat16):
    values = scale * jax.random.normal(own_key, shape, jnp.float32)
    if cuts:
        values = values * level_of(own_key, shape, cuts, -0.22, 0.18)
    return jnp.clip(values, -most, most).astype(held_as)


def setup_inputs(seed: int = 0) -> dict:
    seeds = jax.random.split(jax.random.key(seed), 11)
    volume = draw_volume(jax.random.fold_in(seeds[10], 71), 0)
    amax_history = draw_amax_history(jax.random.fold_in(seeds[10], 71), 0)
    conv_first = gaussian(seeds[2], (27, C1, C1), (27 * C1) ** -0.5, 0.21875)
    conv_second = gaussian(seeds[3], (27, C1, C1), (27 * C1) ** -0.5, 0.21875)
    conv_third = gaussian(seeds[4], (27, C2, C1), (27 * C1) ** -0.5, 0.21875, ((1, 4),))
    conv_fourth = gaussian(seeds[5], (27, C2, C2), (27 * C2) ** -0.5, 0.15625, ((1, 4),))
    gain_fine = jnp.clip(1.0 + 0.1 * jax.random.normal(seeds[6], (2, C1), jnp.float32), 0.5, 1.5)
    shift_fine = jnp.clip(jax.random.uniform(seeds[7], (2, C1), jnp.float32, -0.5, 0.5), -0.5, 0.5)
    gain_coarse = jnp.clip(1.0 + 0.1 * jax.random.normal(seeds[8], (2, C2), jnp.float32), 0.5, 1.5)
    shift_coarse = jnp.clip(jax.random.uniform(seeds[9], (2, C2), jnp.float32, -0.5, 0.5) * level_of(seeds[9], (2, C2), ((1, 4),), -0.4, 0.0), -0.5, 0.5)
    return {"volume": volume, "amax_history": amax_history, "conv_first": conv_first, "conv_second": conv_second, "conv_third": conv_third, "conv_fourth": conv_fourth, "gain_fine": gain_fine, "shift_fine": shift_fine, "gain_coarse": gain_coarse, "shift_coarse": shift_coarse}


norm_eps = 1e-05
leak_slope = 0.01

def convolve(values, weight):
    out_chan = weight.shape[1]
    in_chan = weight.shape[2]
    kernel = jnp.transpose(weight.reshape(3, 3, 3, out_chan, in_chan), (3, 4, 0, 1, 2))
    result = lax.conv_general_dilated(values.astype(jnp.float32)[None], kernel.astype(jnp.float32), (1, 1, 1), 'SAME', dimension_numbers=('NCDHW', 'OIDHW', 'NCDHW'), precision=lax.Precision.HIGHEST)
    return result[0]

def activate(values, gains, offset):
    cell_count = values[0].size
    flat_rows = values.reshape(values.shape[0], -1)
    chan_mean = lax.optimization_barrier(jnp.sum(flat_rows, axis=1)) / cell_count
    spread = lax.optimization_barrier(jnp.sum(flat_rows * flat_rows, axis=1)) / cell_count - chan_mean * chan_mean
    scaling = lax.rsqrt(spread + norm_eps) * gains
    normed = (values - chan_mean[:, None, None, None]) * scaling[:, None, None, None] + offset[:, None, None, None]
    return jnp.where(normed >= 0, normed, leak_slope * normed).astype(jnp.bfloat16)

def limited(values, bound):
    return jnp.clip(values.astype(jnp.float32), -bound, bound).astype(jnp.bfloat16)

def pool_max(values):
    chans, depth_cells, height_cells, width_cells = values.shape
    blocks = values.reshape(chans, depth_cells // 2, 2, height_cells // 2, 2, width_cells // 2, 2)
    return lax.optimization_barrier(jnp.max(blocks, axis=(2, 4, 6)))

def reference(volume, amax_history, conv_first, conv_second, conv_third, conv_fourth, gain_fine, shift_fine, gain_coarse, shift_coarse):
    bounds = lax.optimization_barrier(jnp.max(amax_history, axis=1))

    def single(volume_one):
        first = activate(convolve(limited(volume_one, bounds[0]), conv_first), gain_fine[0], shift_fine[0])
        skip_out = activate(convolve(limited(first, bounds[1]), conv_second), gain_fine[1], shift_fine[1])
        pooled = pool_max(skip_out)
        coarse = activate(convolve(limited(pooled, bounds[2]), conv_third), gain_coarse[0], shift_coarse[0])
        coarse_out = activate(convolve(limited(coarse, bounds[3]), conv_fourth), gain_coarse[1], shift_coarse[1])
        peak_list = jnp.stack([jnp.max(jnp.abs(member.astype(jnp.float32))) for member in (volume_one, first, pooled, coarse)])
        return (skip_out, coarse_out.reshape(coarse_out.shape[0], coarse_out.shape[1], -1), peak_list)
    skip_all, coarse_all, peak_all = lax.map(single, volume)
    return (skip_all, coarse_all, lax.optimization_barrier(jnp.max(peak_all, axis=0)))
```

```python
import functools

import jax
import jax.numpy as jnp
from jax import lax
from jax.experimental import pallas as pl
from jax.experimental.pallas import tpu as pltpu
from jax.sharding import PartitionSpec as P

norm_eps = 1e-05
leak_slope = 0.01
LANES = 128
HALF = LANES // 2
MESH = pl.DeviceIdType.MESH
F32 = jnp.float32
BF16 = jnp.bfloat16
STEPS = ((-1, 0), (1, 0), (0, -1), (0, 1), (-1, -1), (-1, 1), (1, -1), (1, 1))


def iota(shape, dim):
    return lax.broadcasted_iota(jnp.int32, shape, dim)


def lane_row(column, start):
    n = column.shape[0]
    here = iota((n, LANES), 1) == iota((n, LANES), 0) + start
    return jnp.sum(jnp.where(here, column, 0.0), axis=0, keepdims=True)


def to_column(row, n, start):
    shape = (n, row.shape[1])
    here = iota(shape, 1) == iota(shape, 0) + start
    return jnp.sum(jnp.where(here, row, 0.0), axis=1, keepdims=True)


def remote(src, dst, send, recv, where):
    return pltpu.make_async_remote_copy(
        src_ref=src, dst_ref=dst, send_sem=send, recv_sem=recv, device_id=where, device_id_type=MESH
    )


def rounded(v):
    return v.astype(BF16).astype(F32)


def network(sizes, *refs):
    (
        volume, hist_in, c1_in, c2_in, c3_in, c4_in, gf_in, sf_in, gc_in, sc_in,
        skip_out, coarse_out, peak_out,
        given, hist, c1, c2, c3, c4, gf, sf, gc, sc,
        w1, w2, w3, w4, grow, turn, vol, vals1, vals2, stacked, prod,
        pool, vals3, vals4, fin, wide3, wide4, prod3,
        zf0, yf0, co0, zf1, yf1, co1, zf2, yf2, co2, zf3, yf3, co3,
        stat, peak_all,
        in_s, halo_s, halo_r, stat_s, stat_r, w_s, w_r, fin_s, fin_r, pa_s, pa_r,
    ) = refs
    ns, ny, nz = sizes
    zc, yc, ch, xc = vol.shape
    hz, pairs = zc // 2, yc // 4
    oc = c3.shape[1]
    wc = ny * oc
    group = ny * nz
    my_s, my_y, my_z = lax.axis_index("sample"), lax.axis_index("sy"), lax.axis_index("sz")
    me = my_y * nz + my_z

    def member(index):
        return {"sy": index // nz, "sz": lax.rem(index, nz)}

    barrier = pltpu.get_barrier_semaphore()
    for k in range(1, group):
        pl.semaphore_signal(barrier, inc=1, device_id=member(lax.rem(me + k, group)), device_id_type=MESH)
    for k in range(1, ns):
        pl.semaphore_signal(
            barrier, inc=1, device_id={"sample": lax.rem(my_s + k, ns)}, device_id_type=MESH
        )

    pairs_in = (
        (volume, given), (hist_in, hist), (c1_in, c1), (c2_in, c2), (c3_in, c3), (c4_in, c4),
        (gf_in, gf), (sf_in, sf), (gc_in, gc), (sc_in, sc),
    )
    fetch = [pltpu.make_async_copy(a, b, in_s.at[i]) for i, (a, b) in enumerate(pairs_in)]
    for copy in fetch:
        copy.start()

    def inside(dz, dy):
        z, y = my_z + dz, my_y + dy
        return (z >= 0) & (z < nz) & (y >= 0) & (y < ny)

    class Halo:
        def __init__(self, layer, src, zface, yface, corner):
            self.layer, self.src = layer, src
            self.zface, self.yface, self.corner = zface, yface, corner

        def landing(self, d):
            dz, dy = STEPS[d]
            if dy == 0:
                return self.zface.at[int(dz < 0)]
            if dz == 0:
                return self.yface.at[int(dy < 0)]
            return self.corner.at[int(dz < 0) * 2 + int(dy < 0)]

        def copy(self, d):
            dz, dy = STEPS[d]
            planes, rows = self.src.shape[0], self.src.shape[1]
            zi = 0 if dz < 0 else planes - 1
            yi = 0 if dy < 0 else rows - 1
            if dy == 0:
                src = self.src.at[zi]
            elif dz == 0:
                src = self.src.at[:, yi]
            else:
                src = self.src.at[zi, yi]
            where = {"sy": jnp.clip(my_y + dy, 0, ny - 1), "sz": jnp.clip(my_z + dz, 0, nz - 1)}
            at = self.layer, d
            return remote(src, self.landing(d), halo_s.at[at], halo_r.at[at], where)

        def start(self):
            for d, (dz, dy) in enumerate(STEPS):
                @pl.when(inside(dz, dy))
                def _():
                    self.copy(d).start()

        def blank(self):
            for d, (dz, dy) in enumerate(STEPS):
                @pl.when(jnp.logical_not(inside(-dz, -dy)))
                def _():
                    dst = self.landing(d)
                    dst[...] = jnp.zeros(dst.shape, dst.dtype)

        def wait(self, flat):
            for d, (dz, dy) in enumerate(STEPS):
                if (dz == 0) != flat:
                    continue

                @pl.when(inside(-dz, -dy))
                def _():
                    self.copy(d).wait_recv()

                @pl.when(inside(dz, dy))
                def _():
                    self.copy(d).wait_send()

    halo0 = Halo(0, vol, zf0, yf0, co0)
    halo1 = Halo(1, vals1, zf1, yf1, co1)
    halo2 = Halo(2, pool, zf2, yf2, co2)
    halo3 = Halo(3, vals3, zf3, yf3, co3)

    fetch[0].wait()
    for z in range(zc):
        turn[z] = given[:, z].astype(F32).reshape(ch * yc, LANES)
    for z in range(zc):
        for y in range(yc):
            vol[z, y] = turn[z, pl.ds(y, ch, yc), :].astype(BF16)
    pl.semaphore_wait(barrier, group - 1 + ns - 1)
    halo0.start()
    for copy in fetch[1:]:
        copy.wait()

    bounds = [jnp.max(hist[l : l + 1, :]) for l in range(4)]
    lane = iota((ch, LANES), 1)

    def limit(layer, dz, dy):
        if dz == 0 and dy == 0:
            return bounds[layer]
        return jnp.where(inside(dz, dy), bounds[layer], 0.0)

    def put(zp, yp, v, bound):
        v = jnp.clip(v, -bound, bound)
        left = jnp.where(lane == 0, 0.0, pltpu.roll(v, 1, 1))
        right = jnp.where(lane == LANES - 1, 0.0, pltpu.roll(v, LANES - 1, 1))
        stacked[zp, yp] = jnp.concatenate([left, v, right], axis=0).astype(BF16)

    def fine_inner(src, value, layer):
        def plane(z, top):
            for y in range(yc):
                v = value(src[z, y])
                top = jnp.maximum(top, jnp.abs(v))
                put(z + 1, y + 1, v, bounds[layer])
            return top

        top = lax.fori_loop(0, zc, plane, jnp.zeros((ch, LANES), F32))
        return jnp.max(rounded(top))

    def fine_conv(w, halo, value, layer, out):
        def plane(zp, carry):
            for y in range(0, yc, 2):
                rows = [stacked[zp, y + i : y + i + 3].reshape(9 * ch, LANES) for i in range(2)]
                prod[zp, y // 2] = jnp.dot(
                    w[...], jnp.concatenate(rows, axis=1), preferred_element_type=F32
                )
            return carry

        halo.wait(True)
        for side in range(2):
            bound = limit(layer, 0, 2 * side - 1)
            for z in range(zc):
                put(z + 1, side * (yc + 1), value(halo.yface[side, z]), bound)
        lax.fori_loop(1, zc + 1, plane, 0)
        halo.wait(False)
        for side in range(2):
            bound = limit(layer, 2 * side - 1, 0)
            for y in range(yc):
                put(side * (zc + 1), y + 1, value(halo.zface[side, y]), bound)
            for other in range(2):
                bound = limit(layer, 2 * side - 1, 2 * other - 1)
                put(side * (zc + 1), other * (yc + 1), value(halo.corner[side * 2 + other]), bound)
        lax.fori_loop(0, 2, lambda i, carry: plane(i * (zc + 1), carry), 0)

        def total(z, carry):
            s, q = carry
            for y in range(yc // 2):
                v = (
                    prod[z, y, 0:ch, :]
                    + prod[z + 1, y, ch : 2 * ch, :]
                    + prod[z + 2, y, 2 * ch : 3 * ch, :]
                )
                for i in range(2):
                    part = v[:, i * LANES : (i + 1) * LANES]
                    out[z, 2 * y + i] = part
                    s, q = s + part, q + part * part
            return s, q

        zero = jnp.zeros((ch, LANES), F32)
        return lax.fori_loop(0, zc, total, (zero, zero))

    class Stats:
        def __init__(self, phase, rows):
            self.phase, self.count = phase, len(rows)
            for r, row in enumerate(rows):
                stat[phase, me, r : r + 1, :] = row
            for k in sorted(range(1, group), key=lambda k: -min(k % nz, -k % nz)):
                self.copy(k, True).start()

        def copy(self, k, mine):
            other = lax.rem(me + k, group)
            at = me if mine else other
            ref = stat.at[self.phase, at, pl.ds(0, self.count)]
            sems = stat_s.at[self.phase, k], stat_r.at[self.phase, at]
            return remote(ref, ref, *sems, member(other))

        def wait(self):
            for k in range(1, group):
                self.copy(k, False).wait_recv()
                self.copy(k, True).wait_send()

        def rows(self, r):
            return [stat[self.phase, i, r : r + 1, :] for i in range(group)]

    def tree(op, parts):
        while len(parts) > 1:
            parts = [op(*parts[i : i + 2]) if i + 1 < len(parts) else parts[i] for i in range(0, len(parts), 2)]
        return parts[0]

    def sums_row(s, q):
        return lane_row(jnp.sum(s, axis=1, keepdims=True), 0) + lane_row(
            jnp.sum(q, axis=1, keepdims=True), HALF
        )

    def norm_of(total, n, start, cells, gain, shift):
        mean = to_column(total, n, start) / cells
        spread = to_column(total, n, start + HALF) / cells - mean * mean
        scaling = lax.rsqrt(spread + norm_eps) * gain
        return mean, scaling, shift

    def act_of(norm, wide=True):
        n = norm[0].shape[0]
        mean, scaling, offset = (
            tuple(jnp.broadcast_to(a, (n, LANES)) for a in norm) if wide else norm
        )

        def act(v):
            normed = (v - mean) * scaling + offset
            return jnp.maximum(normed, leak_slope * normed)

        return act

    def build(dst, taps):
        out = taps.shape[1]
        for a in range(3):
            parts = [taps[9 * a + k].astype(F32) for k in range(9)]
            dst[a * out : (a + 1) * out, :] = jnp.concatenate(parts, axis=1).astype(BF16)

    def plain(v):
        return v.astype(F32)

    build(w1, c1)
    halo0.blank()
    peak0 = fine_inner(vol, plain, 0)
    build(w2, c2)
    build(w3.at[my_y], c3)
    build(w4.at[my_y], c4)
    own_gain = to_column(gc[0:1, :], oc, 0)
    own_shift = to_column(sc[0:1, :], oc, 0)
    grow[my_y, 0:1, :] = lane_row(own_gain, my_y * oc) + lane_row(own_shift, HALF + my_y * oc)
    for halo in (halo1, halo2, halo3):
        halo.blank()
    s, q = fine_conv(w1, halo0, plain, 0, vals1)
    stats = Stats(0, [sums_row(s, q)])
    halo1.start()

    def gathers(mine):
        out = []
        for k in range(1, ny):
            other = lax.rem(my_y + k, ny)
            at = my_y if mine else other
            for i, buf in enumerate((grow, w3, w4)):
                out.append(remote(buf.at[at], buf.at[at], w_s.at[i, k], w_r.at[i, at], {"sy": other}))
        return out

    for copy in gathers(True):
        copy.start()
    fine_cells = float(zc * nz * yc * ny * xc)

    def fine_norm(layer):
        total = tree(jnp.add, stats.rows(0))
        gain, shift = to_column(gf[layer : layer + 1, :], ch, 0), to_column(sf[layer : layer + 1, :], ch, 0)
        return norm_of(total, ch, 0, fine_cells, gain, shift)

    stats.wait()
    act = act_of(fine_norm(0))

    peak1 = fine_inner(vals1, act, 1)
    s, q = fine_conv(w2, halo1, act, 1, vals2)
    stats = Stats(1, [sums_row(s, q)])

    pick = jnp.where(iota((2 * LANES, LANES), 0) == 2 * iota((2 * LANES, LANES), 1), 1.0, 0.0).astype(BF16)
    for z in range(hz):
        for t in range(pairs):
            found = []
            for i in range(2):
                y = 4 * t + 2 * i
                block = [vals2[2 * z + a, y + b] for a in range(2) for b in range(2)]
                m = tree(jnp.maximum, block)
                found.append(jnp.maximum(m, pltpu.roll(m, LANES - 1, 1)))
            m = jnp.concatenate(found, axis=1)
            high = rounded(m)
            middle = rounded(m - high)
            low = m - high - middle
            split = jnp.concatenate([high, middle, low], axis=0).astype(BF16)
            r = jnp.dot(split, pick, preferred_element_type=F32)
            pool[z, t] = r[0:ch] + r[ch : 2 * ch] + r[2 * ch : 3 * ch]
    halo2.start()
    for mine, theirs in zip(gathers(True), gathers(False)):
        theirs.wait_recv()
        mine.wait_send()
    stats.wait()
    act_skip = act_of(fine_norm(1))

    def widen(n, zp, load, wide):
        where = iota((n, LANES), 1)
        column = lax.rem(where, HALF)
        below = iota((3 * n, LANES), 1) < HALF
        xs, us = [], []
        for tp in range(pairs + 2):
            v = load(tp)
            left = jnp.where(column == 0, 0.0, pltpu.roll(v, 1, 1))
            right = jnp.where(column == HALF - 1, 0.0, pltpu.roll(v, LANES - 1, 1))
            x = jnp.concatenate([left, v, right], axis=0)
            xs.append(x)
            us.append(pltpu.roll(x, HALF, 1))
        for t in range(pairs):
            cols = slice(t * LANES, (t + 1) * LANES)
            rows = (
                jnp.where(below, us[t], us[t + 1]), xs[t + 1], jnp.where(below, us[t + 1], us[t + 2])
            )
            for b, part in enumerate(rows):
                wide[zp, b * 3 * n : (b + 1) * 3 * n, cols] = part.astype(BF16)

    def coarse_conv(w, n, halo, act, layer, wide, store):
        top = jnp.zeros((n, LANES), F32)

        def inner(zp):
            def load(tp):
                nonlocal top
                if tp in (0, pairs + 1):
                    side = int(tp > 0)
                    bound = limit(layer, 0, 2 * side - 1)
                    v = act(halo.yface[side, zp - 1])
                else:
                    bound = bounds[layer]
                    v = act(halo.src[zp - 1, tp - 1])
                    top = jnp.maximum(top, jnp.abs(v))
                return jnp.clip(v, -bound, bound)

            return load

        def outer(side):
            def load(tp):
                if tp in (0, pairs + 1):
                    other = int(tp > 0)
                    bound = limit(layer, 2 * side - 1, 2 * other - 1)
                    v = act(halo.corner[side * 2 + other])
                else:
                    bound = limit(layer, 2 * side - 1, 0)
                    v = act(halo.zface[side, tp - 1])
                return jnp.clip(v, -bound, bound)

            return load

        def plane(zp, load):
            widen(n, zp, load, wide)
            weights = w[...].reshape(3 * wc, 9 * n)
            prod3[zp] = jnp.dot(weights, wide[zp], preferred_element_type=F32)

        halo.wait(True)
        for zp in range(1, hz + 1):
            plane(zp, inner(zp))
        halo.wait(False)
        for side in range(2):
            plane(side * (hz + 1), outer(side))

        parts = []
        for y in range(ny):
            base = 3 * oc * y
            s = q = jnp.zeros((oc, LANES), F32)
            most = least = None
            for z in range(hz):
                for t in range(pairs):
                    cols = slice(t * LANES, (t + 1) * LANES)
                    v = (
                        prod3[z, base : base + oc, cols]
                        + prod3[z + 1, base + oc : base + 2 * oc, cols]
                        + prod3[z + 2, base + 2 * oc : base + 3 * oc, cols]
                    )
                    store(y, z, t, v)
                    s, q = s + v, q + v * v
                    most = v if most is None else jnp.maximum(most, v)
                    least = -v if least is None else jnp.maximum(least, -v)
            parts.append((s, q, most, least))
        joined = [jnp.concatenate(list(p), axis=0) for p in zip(*parts)]
        return joined, jnp.max(rounded(top))

    def store3(y, z, t, v):
        vals3[z, t, y * oc : (y + 1) * oc, :] = v

    def store4(y, z, t, v):
        vals4[y, z, t] = v

    (s, q, most, least), peak2 = coarse_conv(w3, ch, halo2, act_skip, 2, wide3, store3)
    at = iota((1, LANES), 1)
    row = jnp.zeros((1, LANES), F32)
    for i, value in enumerate((peak0, peak1, peak2)):
        row = jnp.where(at == i, value, row)
    ends = lane_row(jnp.max(most, axis=1, keepdims=True), 0) + lane_row(
        jnp.max(least, axis=1, keepdims=True), HALF
    )
    stats = Stats(2, [sums_row(s, q), ends, row])
    halo3.start()

    for z in range(zc):
        for y in range(yc):
            turn[z, pl.ds(y, ch, yc), :] = act_skip(vals2[z, y])
    for z in range(zc):
        skip_out[:, z] = turn[z].reshape(ch, yc, LANES).astype(BF16)

    coarse_cells = float(hz * nz * pairs * ny * LANES)
    gains = tree(jnp.add, [grow[y, 0:1, :] for y in range(ny)])
    stats.wait()
    third = stats
    total = tree(jnp.add, third.rows(0))
    norm3 = norm_of(total, wc, 0, coarse_cells, to_column(gains, wc, 0), to_column(gains, wc, HALF))
    (s, q, _, _), _ = coarse_conv(w4, wc, halo3, act_of(norm3), 3, wide4, store4)
    stats = Stats(3, [sums_row(s, q)])

    def blocks(mine):
        out = []
        for k in range(1, ny):
            other = lax.rem(my_y + k, ny)
            at = my_y if mine else other
            out.append(remote(vals4.at[other], fin.at[at], fin_s.at[k], fin_r.at[at], {"sy": other}))
        return out

    for copy in blocks(True):
        copy.start()
    fin[my_y] = vals4[my_y]

    ends = tree(jnp.maximum, third.rows(1))
    act = act_of(norm3, False)
    high, low = act(to_column(ends, wc, 0)), act(-to_column(ends, wc, HALF))
    peak3 = jnp.max(rounded(jnp.maximum(jnp.abs(high), jnp.abs(low))))
    row = jnp.where(at == 3, peak3, tree(jnp.maximum, third.rows(2)))
    peak_all[my_s, 0:1, :] = row

    def across(k, mine):
        other = lax.rem(my_s + k, ns)
        slot = my_s if mine else other
        ref = peak_all.at[slot, pl.ds(0, 1)]
        return remote(ref, ref, pa_s.at[k], pa_r.at[slot], {"sample": other})

    for k in range(1, ns):
        across(k, True).start()

    own_gain = to_column(gc[1:2, :], oc, 0)
    own_shift = to_column(sc[1:2, :], oc, 0)
    for mine, theirs in zip(blocks(True), blocks(False)):
        theirs.wait_recv()
        mine.wait_send()
    stats.wait()
    total = tree(jnp.add, stats.rows(0))
    act = act_of(norm_of(total, oc, my_y * oc, coarse_cells, own_gain, own_shift))
    for z in range(hz):
        cells = [act(fin[y, z, t]) for y in range(ny) for t in range(pairs)]
        coarse_out[:, z, :] = jnp.concatenate(cells, axis=1).astype(BF16)

    for k in range(1, ns):
        across(k, False).wait_recv()
        across(k, True).wait_send()
    row = tree(jnp.maximum, [peak_all[i, 0:1, :] for i in range(ns)])
    for i in range(4):
        peak_out[i] = jnp.max(jnp.where(at == i, row, 0.0))


def per_device(sizes, volume, hist, c1, c2, c3, c4, gf, sf, gc, sc):
    ns, ny, nz = sizes
    _, ch, zc, yc, xc = volume.shape
    oc = c3.shape[1]
    wc = ny * oc
    hz, pairs = zc // 2, yc // 4
    flat = pairs * ny * LANES
    group = ny * nz
    assert xc == LANES and zc % 2 == 0 and yc % 4 == 0 and wc <= HALF

    args = (volume[0], hist, c1, c2, c3, c4, gf, sf, gc, sc)
    vmem = pl.BlockSpec(memory_space=pltpu.VMEM)
    dma = pltpu.SemaphoreType.DMA

    def faces(planes, rows, n, dtype):
        return [
            pltpu.VMEM((2, rows, n, LANES), dtype),
            pltpu.VMEM((2, planes, n, LANES), dtype),
            pltpu.VMEM((4, n, LANES), dtype),
        ]

    skip, coarse, peaks = pl.pallas_call(
        functools.partial(network, sizes),
        out_shape=(
            jax.ShapeDtypeStruct((ch, zc, yc, xc), BF16),
            jax.ShapeDtypeStruct((oc, hz, flat), BF16),
            jax.ShapeDtypeStruct((4,), F32),
        ),
        in_specs=[pl.BlockSpec(memory_space=IN_SPACE)] * len(args),
        out_specs=(vmem, vmem, pl.BlockSpec(memory_space=pltpu.SMEM)),
        scratch_shapes=[
            *[pltpu.VMEM(a.shape, a.dtype) for a in args],
            pltpu.VMEM((3 * ch, 9 * ch), BF16),
            pltpu.VMEM((3 * ch, 9 * ch), BF16),
            pltpu.VMEM((ny, 3 * oc, 9 * ch), BF16),
            pltpu.VMEM((ny, 3 * oc, 9 * wc), BF16),
            pltpu.VMEM((ny, 8, LANES), F32),
            pltpu.VMEM((zc, ch * yc, LANES), F32),
            pltpu.VMEM((zc, yc, ch, LANES), BF16),
            pltpu.VMEM((zc, yc, ch, LANES), F32),
            pltpu.VMEM((zc, yc, ch, LANES), F32),
            pltpu.VMEM((zc + 2, yc + 2, 3 * ch, LANES), BF16),
            pltpu.VMEM((zc + 2, yc // 2, 3 * ch, 2 * LANES), F32),
            pltpu.VMEM((hz, pairs, ch, LANES), F32),
            pltpu.VMEM((hz, pairs, wc, LANES), F32),
            pltpu.VMEM((ny, hz, pairs, oc, LANES), F32),
            pltpu.VMEM((ny, hz, pairs, oc, LANES), F32),
            pltpu.VMEM((hz + 2, 9 * ch, pairs * LANES), BF16),
            pltpu.VMEM((hz + 2, 9 * wc, pairs * LANES), BF16),
            pltpu.VMEM((hz + 2, 3 * wc, pairs * LANES), F32),
            *faces(zc, yc, ch, BF16),
            *faces(zc, yc, ch, F32),
            *faces(hz, pairs, ch, F32),
            *faces(hz, pairs, wc, F32),
            pltpu.VMEM((4, group, 8, LANES), F32),
            pltpu.VMEM((ns, 8, LANES), F32),
            dma((len(args),)),
            dma((4, 8)),
            dma((4, 8)),
            dma((4, group)),
            dma((4, group)),
            dma((3, ny)),
            dma((3, ny)),
            dma((ny,)),
            dma((ny,)),
            dma((ns,)),
            dma((ns,)),
        ],
        compiler_params=pltpu.CompilerParams(
            collective_id=0, has_side_effects=True, vmem_limit_bytes=VMEM_BYTES
        ),
    )(*args)

    def finish(a, b, c, oa, ob, oc_):
        oa[...] = a[...]
        ob[...] = b[...]
        for i in range(4):
            oc_[i] = c[i]

    smem = pl.BlockSpec(memory_space=pltpu.SMEM)
    skip, coarse, peaks = pl.pallas_call(
        finish,
        out_shape=tuple(jax.ShapeDtypeStruct(a.shape, a.dtype) for a in (skip, coarse, peaks)),
        in_specs=[vmem, vmem, smem],
        out_specs=(vmem, vmem, smem),
        compiler_params=pltpu.CompilerParams(vmem_limit_bytes=FINISH_BYTES),
    )(skip, coarse, peaks)
    return skip[None], coarse[None], peaks


IN_SPACE = pltpu.HBM
VMEM_BYTES = 56 * 1024 * 1024
FINISH_BYTES = 56 * 1024 * 1024


def solution(mesh):
    sizes = (mesh.shape["sample"], mesh.shape["sy"], mesh.shape["sz"])
    return jax.shard_map(
        functools.partial(per_device, sizes),
        mesh=mesh,
        in_specs=(
            P("sample", None, "sz", "sy", None),
            P(),
            P(),
            P(),
            P(None, "sy", None),
            P(None, "sy", None),
            P(),
            P(),
            P(None, "sy"),
            P(None, "sy"),
        ),
        out_specs=(P("sample", None, "sz", "sy", None), P("sample", "sy", "sz", None), P()),
        check_vma=False,
    )
```

```python
import functools

import jax
import jax.numpy as jnp
from jax import lax
from jax.experimental import pallas as pl
from jax.experimental.pallas import tpu as pltpu
from jax.sharding import PartitionSpec as P

norm_eps = 1e-05
leak_slope = 0.01
LANES = 128
HALF = LANES // 2
MESH = pl.DeviceIdType.MESH
F32 = jnp.float32
BF16 = jnp.bfloat16
STEPS = ((-1, 0), (1, 0), (0, -1), (0, 1), (-1, -1), (-1, 1), (1, -1), (1, 1))


def iota(shape, dim):
    return lax.broadcasted_iota(jnp.int32, shape, dim)


def lane_row(column, start):
    n = column.shape[0]
    here = iota((n, LANES), 1) == iota((n, LANES), 0) + start
    return jnp.sum(jnp.where(here, column, 0.0), axis=0, keepdims=True)


def to_column(row, n, start):
    shape = (n, row.shape[1])
    here = iota(shape, 1) == iota(shape, 0) + start
    return jnp.sum(jnp.where(here, row, 0.0), axis=1, keepdims=True)


def remote(src, dst, send, recv, where):
    return pltpu.make_async_remote_copy(
        src_ref=src, dst_ref=dst, send_sem=send, recv_sem=recv, device_id=where, device_id_type=MESH
    )


def rounded(v):
    return v.astype(BF16).astype(F32)


def network(sizes, *refs):
    (
        volume, hist_in, c1_in, c2_in, c3_in, c4_in, gf_in, sf_in, gc_in, sc_in,
        skip_out, coarse_out, peak_out,
        given, hist, c1, c2, c3, c4, gf, sf, gc, sc,
        w1, w2, w3, w4, grow, turn, vol, vals1, vals2, stacked, prod,
        pool, vals3, vals4, fin, wide3, wide4, prod3,
        zf0, yf0, co0, zf1, yf1, co1, zf2, yf2, co2, zf3, yf3, co3,
        stat, peak_all,
        in_s, halo_s, halo_r, stat_s, stat_r, w_s, w_r, fin_s, fin_r, pa_s, pa_r,
    ) = refs
    ns, ny, nz = sizes
    zc, yc, ch, xc = vol.shape
    hz, pairs = zc // 2, yc // 4
    oc = c3.shape[1]
    wc = ny * oc
    group = ny * nz
    my_s, my_y, my_z = lax.axis_index("sample"), lax.axis_index("sy"), lax.axis_index("sz")
    me = my_y * nz + my_z

    pairs_in = (
        (volume, given), (hist_in, hist), (c1_in, c1), (c2_in, c2), (c3_in, c3), (c4_in, c4),
        (gf_in, gf), (sf_in, sf), (gc_in, gc), (sc_in, sc),
    )
    fetch = [pltpu.make_async_copy(a, b, in_s.at[i]) for i, (a, b) in enumerate(pairs_in)]
    for copy in fetch:
        copy.start()

    def ahead(index, k, count):
        index = index + k
        return jnp.where(index >= count, index - count, index)

    ys = [my_y] + [ahead(my_y, k, ny) for k in range(1, ny)]
    zs = [my_z] + [ahead(my_z, k, nz) for k in range(1, nz)]
    far = sorted(range(1, group), key=lambda k: -min(k % nz, -k % nz))

    def member(k):
        return {"sy": ys[k // nz], "sz": zs[k % nz]}

    def slot_of(k):
        return ys[k // nz] * nz + zs[k % nz]

    barrier = pltpu.get_barrier_semaphore()
    for k in far:
        pl.semaphore_signal(barrier, inc=1, device_id=member(k), device_id_type=MESH)
    for k in range(1, ns):
        pl.semaphore_signal(
            barrier, inc=1, device_id={"sample": ahead(my_s, k, ns)}, device_id_type=MESH
        )

    def inside(dz, dy):
        z, y = my_z + dz, my_y + dy
        return (z >= 0) & (z < nz) & (y >= 0) & (y < ny)

    class Halo:
        def __init__(self, layer, src, zface, yface, corner):
            self.layer, self.src = layer, src
            self.zface, self.yface, self.corner = zface, yface, corner

        def landing(self, d):
            dz, dy = STEPS[d]
            if dy == 0:
                return self.zface.at[int(dz < 0)]
            if dz == 0:
                return self.yface.at[int(dy < 0)]
            return self.corner.at[int(dz < 0) * 2 + int(dy < 0)]

        def copy(self, d):
            dz, dy = STEPS[d]
            planes, rows = self.src.shape[0], self.src.shape[1]
            zi = 0 if dz < 0 else planes - 1
            yi = 0 if dy < 0 else rows - 1
            if dy == 0:
                src = self.src.at[zi]
            elif dz == 0:
                src = self.src.at[:, yi]
            else:
                src = self.src.at[zi, yi]
            where = {"sy": jnp.clip(my_y + dy, 0, ny - 1), "sz": jnp.clip(my_z + dz, 0, nz - 1)}
            at = self.layer, d
            return remote(src, self.landing(d), halo_s.at[at], halo_r.at[at], where)

        def start(self):
            for d, (dz, dy) in enumerate(STEPS):
                @pl.when(inside(dz, dy))
                def _():
                    self.copy(d).start()

        def blank(self):
            for d, (dz, dy) in enumerate(STEPS):
                @pl.when(jnp.logical_not(inside(-dz, -dy)))
                def _():
                    dst = self.landing(d)
                    dst[...] = jnp.zeros(dst.shape, dst.dtype)

        def wait(self, flat):
            for d, (dz, dy) in enumerate(STEPS):
                if (dz == 0) != flat:
                    continue

                @pl.when(inside(-dz, -dy))
                def _():
                    self.copy(d).wait_recv()

                @pl.when(inside(dz, dy))
                def _():
                    self.copy(d).wait_send()

    halo0 = Halo(0, vol, zf0, yf0, co0)
    halo1 = Halo(1, vals1, zf1, yf1, co1)
    halo2 = Halo(2, pool, zf2, yf2, co2)
    halo3 = Halo(3, vals3, zf3, yf3, co3)

    fetch[0].wait()
    for z in range(zc):
        turn[z] = given[:, z].astype(F32).reshape(ch * yc, LANES)
    for z in range(zc):
        for y in range(yc):
            vol[z, y] = turn[z, pl.ds(y, ch, yc), :].astype(BF16)
    pl.semaphore_wait(barrier, group - 1 + ns - 1)
    halo0.start()
    for copy in fetch[1:]:
        copy.wait()

    bounds = [jnp.max(hist[l : l + 1, :]) for l in range(4)]
    lane = iota((ch, LANES), 1)

    def limit(layer, dz, dy):
        if dz == 0 and dy == 0:
            return bounds[layer]
        return jnp.where(inside(dz, dy), bounds[layer], 0.0)

    def put(zp, yp, v, bound):
        v = jnp.clip(v, -bound, bound)
        left = jnp.where(lane == 0, 0.0, pltpu.roll(v, 1, 1))
        right = jnp.where(lane == LANES - 1, 0.0, pltpu.roll(v, LANES - 1, 1))
        stacked[zp, yp] = jnp.concatenate([left, v, right], axis=0).astype(BF16)

    def fine_inner(src, value, layer):
        def plane(z, top):
            for y in range(yc):
                v = value(src[z, y])
                top = jnp.maximum(top, jnp.abs(v))
                put(z + 1, y + 1, v, bounds[layer])
            return top

        top = lax.fori_loop(0, zc, plane, jnp.zeros((ch, LANES), F32), unroll=True)
        return jnp.max(rounded(top))

    def fine_conv(w, halo, value, layer, out):
        half = yc // 2

        def tiles(zp, found):
            for t in found:
                rows = [stacked[zp, y : y + 3].reshape(9 * ch, LANES) for y in (2 * t, 2 * t + 1)]
                prod[zp, t] = jnp.dot(
                    w[...], jnp.concatenate(rows, axis=1), preferred_element_type=F32
                )

        def total(z, carry):
            s, q = carry
            for t in range(half):
                v = (
                    prod[z, t, 0:ch, :]
                    + prod[z + 1, t, ch : 2 * ch, :]
                    + prod[z + 2, t, 2 * ch : 3 * ch, :]
                )
                for i in range(2):
                    part = v[:, i * LANES : (i + 1) * LANES]
                    out[z, 2 * t + i] = part
                    s, q = s + part, q + part * part
            return s, q

        for zp in range(1, zc + 1):
            tiles(zp, range(1, half - 1))
        halo.wait(True)
        for side in range(2):
            bound = limit(layer, 0, 2 * side - 1)
            for z in range(zc):
                put(z + 1, side * (yc + 1), value(halo.yface[side, z]), bound)
        for zp in range(1, zc + 1):
            tiles(zp, (0, half - 1))
        carry = jnp.zeros((ch, LANES), F32), jnp.zeros((ch, LANES), F32)
        for z in range(1, zc - 1):
            carry = total(z, carry)
        halo.wait(False)
        for side in range(2):
            bound = limit(layer, 2 * side - 1, 0)
            for y in range(yc):
                put(side * (zc + 1), y + 1, value(halo.zface[side, y]), bound)
            for other in range(2):
                bound = limit(layer, 2 * side - 1, 2 * other - 1)
                put(side * (zc + 1), other * (yc + 1), value(halo.corner[side * 2 + other]), bound)
            tiles(side * (zc + 1), range(half))
        for z in (0, zc - 1):
            carry = total(z, carry)
        return carry

    class Stats:
        def __init__(self, phase, rows):
            self.phase, self.count = phase, len(rows)
            for r, row in enumerate(rows):
                stat[phase, me, r : r + 1, :] = row
            for k in far:
                self.copy(k, True).start()

        def copy(self, k, mine):
            at = me if mine else slot_of(k)
            ref = stat.at[self.phase, at, pl.ds(0, self.count)]
            sems = stat_s.at[self.phase, k], stat_r.at[self.phase, at]
            return remote(ref, ref, *sems, member(k))

        def wait(self):
            for k in range(1, group):
                self.copy(k, False).wait_recv()
                self.copy(k, True).wait_send()

        def rows(self, r):
            return [stat[self.phase, i, r : r + 1, :] for i in range(group)]

    def tree(op, parts):
        while len(parts) > 1:
            parts = [op(*parts[i : i + 2]) if i + 1 < len(parts) else parts[i] for i in range(0, len(parts), 2)]
        return parts[0]

    def sums_row(s, q):
        return lane_row(jnp.sum(s, axis=1, keepdims=True), 0) + lane_row(
            jnp.sum(q, axis=1, keepdims=True), HALF
        )

    def norm_of(total, n, start, cells, gain, shift):
        mean = to_column(total, n, start) / cells
        spread = to_column(total, n, start + HALF) / cells - mean * mean
        scaling = lax.rsqrt(spread + norm_eps) * gain
        return mean, scaling, shift

    def act_of(norm, wide=True):
        n = norm[0].shape[0]
        mean, scaling, offset = (
            tuple(jnp.broadcast_to(a, (n, LANES)) for a in norm) if wide else norm
        )

        def act(v, rows=slice(None)):
            normed = (v - mean[rows]) * scaling[rows] + offset[rows]
            return jnp.maximum(normed, leak_slope * normed)

        return act

    def build(dst, taps):
        out = taps.shape[1]
        for a in range(3):
            parts = [taps[9 * a + k].astype(F32) for k in range(9)]
            dst[a * out : (a + 1) * out, :] = jnp.concatenate(parts, axis=1).astype(BF16)

    def plain(v):
        return v.astype(F32)

    build(w1, c1)
    halo0.blank()
    peak0 = fine_inner(vol, plain, 0)
    build(w2, c2)
    build(w3.at[my_y], c3)
    build(w4.at[my_y], c4)
    own_gain = to_column(gc[0:1, :], oc, 0)
    own_shift = to_column(sc[0:1, :], oc, 0)
    grow[my_y, 0:1, :] = lane_row(own_gain, my_y * oc) + lane_row(own_shift, HALF + my_y * oc)
    for halo in (halo1, halo2, halo3):
        halo.blank()
    s, q = fine_conv(w1, halo0, plain, 0, vals1)
    stats = Stats(0, [sums_row(s, q)])
    halo1.start()

    def gathers(mine):
        out = []
        for k in range(1, ny):
            other = ys[k]
            at = my_y if mine else other
            for i, buf in enumerate((grow, w3, w4)):
                out.append(remote(buf.at[at], buf.at[at], w_s.at[i, k], w_r.at[i, at], {"sy": other}))
        return out

    for copy in gathers(True):
        copy.start()
    fine_cells = float(zc * nz * yc * ny * xc)

    def fine_norm(layer):
        total = tree(jnp.add, stats.rows(0))
        gain, shift = to_column(gf[layer : layer + 1, :], ch, 0), to_column(sf[layer : layer + 1, :], ch, 0)
        return norm_of(total, ch, 0, fine_cells, gain, shift)

    stats.wait()
    act = act_of(fine_norm(0))

    peak1 = fine_inner(vals1, act, 1)
    s, q = fine_conv(w2, halo1, act, 1, vals2)
    stats = Stats(1, [sums_row(s, q)])

    pick = jnp.where(iota((2 * LANES, LANES), 0) == 2 * iota((2 * LANES, LANES), 1), 1.0, 0.0).astype(BF16)
    for z in range(hz):
        for t in range(pairs):
            found = []
            for i in range(2):
                y = 4 * t + 2 * i
                block = [vals2[2 * z + a, y + b] for a in range(2) for b in range(2)]
                m = tree(jnp.maximum, block)
                found.append(jnp.maximum(m, pltpu.roll(m, LANES - 1, 1)))
            m = jnp.concatenate(found, axis=1)
            high = rounded(m)
            middle = rounded(m - high)
            low = m - high - middle
            split = jnp.concatenate([high, middle, low], axis=0).astype(BF16)
            r = jnp.dot(split, pick, preferred_element_type=F32)
            pool[z, t] = r[0:ch] + r[ch : 2 * ch] + r[2 * ch : 3 * ch]
    halo2.start()
    for mine, theirs in zip(gathers(True), gathers(False)):
        theirs.wait_recv()
        mine.wait_send()
    stats.wait()
    act_skip = act_of(fine_norm(1))

    def widen(n, zp, load, wide):
        part = 2 * 8
        where = iota((part, LANES), 1)
        column = lax.rem(where, HALF)
        below = where < HALF
        for r in range(0, n, part):
            xs, us = [], []
            for tp in range(pairs + 2):
                v = load(tp, slice(r, r + part))
                left = jnp.where(column == 0, 0.0, pltpu.roll(v, 1, 1))
                right = jnp.where(column == HALF - 1, 0.0, pltpu.roll(v, LANES - 1, 1))
                xs.append((left, v, right))
                us.append([pltpu.roll(x, HALF, 1) for x in xs[-1]])
            for t in range(pairs):
                cols = slice(t * LANES, (t + 1) * LANES)
                for c in range(3):
                    taps = (
                        jnp.where(below, us[t][c], us[t + 1][c]),
                        xs[t + 1][c],
                        jnp.where(below, us[t + 1][c], us[t + 2][c]),
                    )
                    for b, tap in enumerate(taps):
                        base = (3 * b + c) * n + r
                        wide[zp, base : base + part, cols] = tap.astype(BF16)

    def coarse_conv(w, n, halo, act, layer, wide, store):
        top = jnp.zeros((2 * 8, LANES), F32)

        def inner(zp):
            def load(tp, rows):
                nonlocal top
                if tp in (0, pairs + 1):
                    side = int(tp > 0)
                    bound = limit(layer, 0, 2 * side - 1)
                    v = act(halo.yface[side, zp - 1, rows], rows)
                else:
                    bound = bounds[layer]
                    v = act(halo.src[zp - 1, tp - 1, rows], rows)
                    top = jnp.maximum(top, jnp.abs(v))
                return jnp.clip(v, -bound, bound)

            return load

        def outer(side):
            def load(tp, rows):
                if tp in (0, pairs + 1):
                    other = int(tp > 0)
                    bound = limit(layer, 2 * side - 1, 2 * other - 1)
                    v = act(halo.corner[side * 2 + other, rows], rows)
                else:
                    bound = limit(layer, 2 * side - 1, 0)
                    v = act(halo.zface[side, tp - 1, rows], rows)
                return jnp.clip(v, -bound, bound)

            return load

        def plane(zp, load):
            widen(n, zp, load, wide)
            weights = w[...].reshape(3 * wc, 9 * n)
            prod3[zp] = jnp.dot(weights, wide[zp], preferred_element_type=F32)

        halo.wait(True)
        for zp in range(1, hz + 1):
            plane(zp, inner(zp))
        halo.wait(False)
        for side in range(2):
            plane(side * (hz + 1), outer(side))

        parts = []
        for y in range(ny):
            base = 3 * oc * y
            s = q = jnp.zeros((oc, LANES), F32)
            most = least = None
            for z in range(hz):
                for t in range(pairs):
                    cols = slice(t * LANES, (t + 1) * LANES)
                    v = (
                        prod3[z, base : base + oc, cols]
                        + prod3[z + 1, base + oc : base + 2 * oc, cols]
                        + prod3[z + 2, base + 2 * oc : base + 3 * oc, cols]
                    )
                    store(y, z, t, v)
                    s, q = s + v, q + v * v
                    most = v if most is None else jnp.maximum(most, v)
                    least = -v if least is None else jnp.maximum(least, -v)
            parts.append((s, q, most, least))
        joined = [jnp.concatenate(list(p), axis=0) for p in zip(*parts)]
        return joined, jnp.max(rounded(top))

    def store3(y, z, t, v):
        vals3[z, t, y * oc : (y + 1) * oc, :] = v

    def store4(y, z, t, v):
        vals4[y, z, t] = v

    (s, q, most, least), peak2 = coarse_conv(w3, ch, halo2, act_skip, 2, wide3, store3)
    at = iota((1, LANES), 1)
    row = jnp.zeros((1, LANES), F32)
    for i, value in enumerate((peak0, peak1, peak2)):
        row = jnp.where(at == i, value, row)
    ends = lane_row(jnp.max(most, axis=1, keepdims=True), 0) + lane_row(
        jnp.max(least, axis=1, keepdims=True), HALF
    )
    stats = Stats(2, [sums_row(s, q), ends, row])
    halo3.start()

    for z in range(zc):
        for y in range(yc):
            turn[z, pl.ds(y, ch, yc), :] = act_skip(vals2[z, y])
    for z in range(zc):
        skip_out[:, z] = turn[z].reshape(ch, yc, LANES).astype(BF16)

    coarse_cells = float(hz * nz * pairs * ny * LANES)
    gains = tree(jnp.add, [grow[y, 0:1, :] for y in range(ny)])
    stats.wait()
    third = stats
    total = tree(jnp.add, third.rows(0))
    norm3 = norm_of(total, wc, 0, coarse_cells, to_column(gains, wc, 0), to_column(gains, wc, HALF))
    (s, q, _, _), _ = coarse_conv(w4, wc, halo3, act_of(norm3), 3, wide4, store4)
    stats = Stats(3, [sums_row(s, q)])

    def blocks(mine):
        out = []
        for k in range(1, ny):
            other = ys[k]
            at = my_y if mine else other
            out.append(remote(vals4.at[other], fin.at[at], fin_s.at[k], fin_r.at[at], {"sy": other}))
        return out

    for copy in blocks(True):
        copy.start()
    fin[my_y] = vals4[my_y]

    ends = tree(jnp.maximum, third.rows(1))
    act = act_of(norm3, False)
    high, low = act(to_column(ends, wc, 0)), act(-to_column(ends, wc, HALF))
    peak3 = jnp.max(rounded(jnp.maximum(jnp.abs(high), jnp.abs(low))))
    row = jnp.where(at == 3, peak3, tree(jnp.maximum, third.rows(2)))
    peak_all[my_s, 0:1, :] = row

    def across(k, mine):
        other = ahead(my_s, k, ns)
        slot = my_s if mine else other
        ref = peak_all.at[slot, pl.ds(0, 1)]
        return remote(ref, ref, pa_s.at[k], pa_r.at[slot], {"sample": other})

    for k in range(1, ns):
        across(k, True).start()

    own_gain = to_column(gc[1:2, :], oc, 0)
    own_shift = to_column(sc[1:2, :], oc, 0)
    for mine, theirs in zip(blocks(True), blocks(False)):
        theirs.wait_recv()
        mine.wait_send()
    stats.wait()
    total = tree(jnp.add, stats.rows(0))
    act = act_of(norm_of(total, oc, my_y * oc, coarse_cells, own_gain, own_shift))
    for z in range(hz):
        cells = [act(fin[y, z, t]) for y in range(ny) for t in range(pairs)]
        coarse_out[:, z, :] = jnp.concatenate(cells, axis=1).astype(BF16)

    for k in range(1, ns):
        across(k, False).wait_recv()
        across(k, True).wait_send()
    row = tree(jnp.maximum, [peak_all[i, 0:1, :] for i in range(ns)])
    peak_out[...] = row[0, 0 : peak_out.shape[0]]


def per_device(sizes, volume, hist, c1, c2, c3, c4, gf, sf, gc, sc):
    ns, ny, nz = sizes
    _, ch, zc, yc, xc = volume.shape
    oc = c3.shape[1]
    wc = ny * oc
    hz, pairs = zc // 2, yc // 4
    flat = pairs * ny * LANES
    group = ny * nz
    assert xc == LANES and zc % 2 == 0 and yc % 4 == 0 and wc <= HALF

    args = (volume[0], hist, c1, c2, c3, c4, gf, sf, gc, sc)
    args = tuple(pltpu.with_memory_space_constraint(x, pltpu.HBM) for x in args)
    vmem = pl.BlockSpec(memory_space=pltpu.VMEM)
    dma = pltpu.SemaphoreType.DMA

    def faces(planes, rows, n, dtype):
        return [
            pltpu.VMEM((2, rows, n, LANES), dtype),
            pltpu.VMEM((2, planes, n, LANES), dtype),
            pltpu.VMEM((4, n, LANES), dtype),
        ]

    skip, coarse, peaks = pl.pallas_call(
        functools.partial(network, sizes),
        out_shape=(
            jax.ShapeDtypeStruct((ch, zc, yc, xc), BF16),
            jax.ShapeDtypeStruct((oc, hz, flat), BF16),
            jax.ShapeDtypeStruct((4,), F32),
        ),
        in_specs=[pl.BlockSpec(memory_space=IN_SPACE)] * len(args),
        out_specs=(vmem, vmem, vmem),
        scratch_shapes=[
            *[pltpu.VMEM(a.shape, a.dtype) for a in args],
            pltpu.VMEM((3 * ch, 9 * ch), BF16),
            pltpu.VMEM((3 * ch, 9 * ch), BF16),
            pltpu.VMEM((ny, 3 * oc, 9 * ch), BF16),
            pltpu.VMEM((ny, 3 * oc, 9 * wc), BF16),
            pltpu.VMEM((ny, 8, LANES), F32),
            pltpu.VMEM((zc, ch * yc, LANES), F32),
            pltpu.VMEM((zc, yc, ch, LANES), BF16),
            pltpu.VMEM((zc, yc, ch, LANES), F32),
            pltpu.VMEM((zc, yc, ch, LANES), F32),
            pltpu.VMEM((zc + 2, yc + 2, 3 * ch, LANES), BF16),
            pltpu.VMEM((zc + 2, yc // 2, 3 * ch, 2 * LANES), F32),
            pltpu.VMEM((hz, pairs, ch, LANES), F32),
            pltpu.VMEM((hz, pairs, wc, LANES), F32),
            pltpu.VMEM((ny, hz, pairs, oc, LANES), F32),
            pltpu.VMEM((ny, hz, pairs, oc, LANES), F32),
            pltpu.VMEM((hz + 2, 9 * ch, pairs * LANES), BF16),
            pltpu.VMEM((hz + 2, 9 * wc, pairs * LANES), BF16),
            pltpu.VMEM((hz + 2, 3 * wc, pairs * LANES), F32),
            *faces(zc, yc, ch, BF16),
            *faces(zc, yc, ch, F32),
            *faces(hz, pairs, ch, F32),
            *faces(hz, pairs, wc, F32),
            pltpu.VMEM((4, group, 8, LANES), F32),
            pltpu.VMEM((ns, 8, LANES), F32),
            dma((len(args),)),
            dma((4, 8)),
            dma((4, 8)),
            dma((4, group)),
            dma((4, group)),
            dma((3, ny)),
            dma((3, ny)),
            dma((ny,)),
            dma((ny,)),
            dma((ns,)),
            dma((ns,)),
        ],
        compiler_params=pltpu.CompilerParams(
            collective_id=0, has_side_effects=True, vmem_limit_bytes=VMEM_BYTES
        ),
    )(*args)

    def finish(*refs):
        copies = [pltpu.make_async_copy(refs[i], refs[3 + i], refs[6].at[i]) for i in range(3)]
        for copy in copies:
            copy.start()
        for copy in copies:
            copy.wait()

    anywhere = pl.BlockSpec(memory_space=pl.ANY)
    skip, coarse, peaks = pl.pallas_call(
        finish,
        out_shape=tuple(jax.ShapeDtypeStruct(a.shape, a.dtype) for a in (skip, coarse, peaks)),
        in_specs=[anywhere] * 3,
        out_specs=[anywhere] * 3,
        scratch_shapes=[dma((3,))],
        compiler_params=pltpu.CompilerParams(vmem_limit_bytes=FINISH_BYTES),
    )(skip, coarse, peaks)
    return skip[None], coarse[None], peaks


IN_SPACE = pltpu.HBM
VMEM_BYTES = 20 * 1024 * 1024
FINISH_BYTES = 4 * 1024 * 1024


def solution(mesh):
    sizes = (mesh.shape["sample"], mesh.shape["sy"], mesh.shape["sz"])
    return jax.shard_map(
        functools.partial(per_device, sizes),
        mesh=mesh,
        in_specs=(
            P("sample", None, "sz", "sy", None),
            P(),
            P(),
            P(),
            P(None, "sy", None),
            P(None, "sy", None),
            P(),
            P(),
            P(None, "sy"),
            P(None, "sy"),
        ),
        out_specs=(P("sample", None, "sz", "sy", None), P("sample", "sy", "sz", None), P()),
        check_vma=False,
    )
```

```python
import functools

import jax
import jax.numpy as jnp
from jax import lax
from jax.experimental import pallas as pl
from jax.experimental.pallas import tpu as pltpu
from jax.sharding import PartitionSpec as P

norm_eps = 1e-05
leak_slope = 0.01
LANES = 128
HALF = LANES // 2
MESH = pl.DeviceIdType.MESH
F32 = jnp.float32
BF16 = jnp.bfloat16
STEPS = ((-1, 0), (1, 0), (0, -1), (0, 1), (-1, -1), (-1, 1), (1, -1), (1, 1))


def iota(shape, dim):
    return lax.broadcasted_iota(jnp.int32, shape, dim)


def lane_row(column, start):
    n = column.shape[0]
    here = iota((n, LANES), 1) == iota((n, LANES), 0) + start
    return jnp.sum(jnp.where(here, column, 0.0), axis=0, keepdims=True)


def to_column(row, n, start):
    shape = (n, row.shape[1])
    here = iota(shape, 1) == iota(shape, 0) + start
    return jnp.sum(jnp.where(here, row, 0.0), axis=1, keepdims=True)


def remote(src, dst, send, recv, where):
    return pltpu.make_async_remote_copy(
        src_ref=src, dst_ref=dst, send_sem=send, recv_sem=recv, device_id=where, device_id_type=MESH
    )


def rounded(v):
    return v.astype(BF16).astype(F32)


def network(sizes, *refs):
    (
        volume, hist_in, c1_in, c2_in, c3_in, c4_in, gf_in, sf_in, gc_in, sc_in,
        skip_out, coarse_out, peak_out,
        given, hist, c1, c2, c3, c4, gf, sf, gc, sc,
        w1, w2, w3, w4, grow, turn, vol, vals1, vals2, stacked, prod,
        pool, vals3, vals4, fin, wide3, wide4, prod3,
        zf0, yf0, co0, zf1, yf1, co1, zf2, yf2, co2, zf3, yf3, co3,
        stat, peak_all,
        in_s, halo_s, halo_r, stat_s, stat_r, w_s, w_r, fin_s, fin_r, pa_s, pa_r,
    ) = refs
    ns, ny, nz = sizes
    zc, yc, ch, xc = vol.shape
    hz, pairs = zc // 2, yc // 4
    oc = c3.shape[1]
    wc = ny * oc
    group = ny * nz
    my_s, my_y, my_z = lax.axis_index("sample"), lax.axis_index("sy"), lax.axis_index("sz")
    me = my_y * nz + my_z

    pairs_in = (
        (volume, given), (hist_in, hist), (c1_in, c1), (c2_in, c2), (c3_in, c3), (c4_in, c4),
        (gf_in, gf), (sf_in, sf), (gc_in, gc), (sc_in, sc),
    )
    fetch = [pltpu.make_async_copy(a, b, in_s.at[i]) for i, (a, b) in enumerate(pairs_in)]
    for copy in fetch:
        copy.start()

    def ahead(index, k, count):
        index = index + k
        return jnp.where(index >= count, index - count, index)

    ys = [my_y] + [ahead(my_y, k, ny) for k in range(1, ny)]
    zs = [my_z]
    for j in range(nz - 1):
        down = nz - 1 - j
        down = jnp.where(down > my_z, down, down - 1)
        zs.append(jnp.where(2 * my_z < nz, down, jnp.where(j < my_z, j, j + 1)))
    far = sorted(range(1, group), key=lambda k: (k % nz == 0, k % nz, -min(k // nz, -(k // nz) % ny)))

    def member(k):
        return {"sy": ys[k // nz], "sz": zs[k % nz]}

    def slot_of(k):
        return ys[k // nz] * nz + zs[k % nz]

    barrier = pltpu.get_barrier_semaphore()
    for k in far:
        pl.semaphore_signal(barrier, inc=1, device_id=member(k), device_id_type=MESH)
    for k in range(1, ns):
        pl.semaphore_signal(
            barrier, inc=1, device_id={"sample": ahead(my_s, k, ns)}, device_id_type=MESH
        )

    def inside(dz, dy):
        z, y = my_z + dz, my_y + dy
        return (z >= 0) & (z < nz) & (y >= 0) & (y < ny)

    class Halo:
        def __init__(self, layer, src, zface, yface, corner):
            self.layer, self.src = layer, src
            self.zface, self.yface, self.corner = zface, yface, corner

        def landing(self, d):
            dz, dy = STEPS[d]
            if dy == 0:
                return self.zface.at[int(dz < 0)]
            if dz == 0:
                return self.yface.at[int(dy < 0)]
            return self.corner.at[int(dz < 0) * 2 + int(dy < 0)]

        def copy(self, d):
            dz, dy = STEPS[d]
            planes, rows = self.src.shape[0], self.src.shape[1]
            zi = 0 if dz < 0 else planes - 1
            yi = 0 if dy < 0 else rows - 1
            if dy == 0:
                src = self.src.at[zi]
            elif dz == 0:
                src = self.src.at[:, yi]
            else:
                src = self.src.at[zi, yi]
            where = {"sy": jnp.clip(my_y + dy, 0, ny - 1), "sz": jnp.clip(my_z + dz, 0, nz - 1)}
            at = self.layer, d
            return remote(src, self.landing(d), halo_s.at[at], halo_r.at[at], where)

        def start(self):
            for d, (dz, dy) in sorted(enumerate(STEPS), key=lambda e: -abs(e[1][0] * e[1][1])):
                @pl.when(inside(dz, dy))
                def _():
                    self.copy(d).start()

        def blank(self):
            for d, (dz, dy) in enumerate(STEPS):
                @pl.when(jnp.logical_not(inside(-dz, -dy)))
                def _():
                    dst = self.landing(d)
                    dst[...] = jnp.zeros(dst.shape, dst.dtype)

        def wait(self, flat):
            for d, (dz, dy) in enumerate(STEPS):
                if (dz == 0) != flat:
                    continue

                @pl.when(inside(-dz, -dy))
                def _():
                    self.copy(d).wait_recv()

                @pl.when(inside(dz, dy))
                def _():
                    self.copy(d).wait_send()

    halo0 = Halo(0, vol, zf0, yf0, co0)
    halo1 = Halo(1, vals1, zf1, yf1, co1)
    halo2 = Halo(2, pool, zf2, yf2, co2)
    halo3 = Halo(3, vals3, zf3, yf3, co3)

    fetch[0].wait()
    for z in range(zc):
        turn[z] = given[:, z].astype(F32).reshape(ch * yc, LANES)
    for z in range(zc):
        for y in range(yc):
            vol[z, y] = turn[z, pl.ds(y, ch, yc), :].astype(BF16)
    pl.semaphore_wait(barrier, group - 1 + ns - 1)
    halo0.start()
    for copy in fetch[1:]:
        copy.wait()

    bounds = [jnp.max(hist[l : l + 1, :]) for l in range(4)]
    lane = iota((ch, LANES), 1)

    def limit(layer, dz, dy):
        if dz == 0 and dy == 0:
            return bounds[layer]
        return jnp.where(inside(dz, dy), bounds[layer], 0.0)

    def put(zp, yp, v, bound):
        v = jnp.clip(v, -bound, bound)
        left = jnp.where(lane == 0, 0.0, pltpu.roll(v, 1, 1))
        right = jnp.where(lane == LANES - 1, 0.0, pltpu.roll(v, LANES - 1, 1))
        stacked[zp, yp] = jnp.concatenate([left, v, right], axis=0).astype(BF16)

    def fine_inner(src, value, layer):
        def plane(z, top):
            for y in range(yc):
                v = value(src[z, y])
                top = jnp.maximum(top, jnp.abs(v))
                put(z + 1, y + 1, v, bounds[layer])
            return top

        top = lax.fori_loop(0, zc, plane, jnp.zeros((ch, LANES), F32), unroll=True)
        return jnp.max(rounded(top))

    def fine_conv(w, halo, value, layer, out):
        half = yc // 2

        def tiles(zp, found):
            for t in found:
                rows = [stacked[zp, y : y + 3].reshape(9 * ch, LANES) for y in (2 * t, 2 * t + 1)]
                prod[zp, t] = jnp.dot(
                    w[...], jnp.concatenate(rows, axis=1), preferred_element_type=F32
                )

        def total(z, carry):
            s, q = carry
            for t in range(half):
                v = (
                    prod[z, t, 0:ch, :]
                    + prod[z + 1, t, ch : 2 * ch, :]
                    + prod[z + 2, t, 2 * ch : 3 * ch, :]
                )
                for i in range(2):
                    part = v[:, i * LANES : (i + 1) * LANES]
                    out[z, 2 * t + i] = part
                    s, q = s + part, q + part * part
            return s, q

        for zp in range(1, zc + 1):
            tiles(zp, range(1, half - 1))
        halo.wait(True)
        for side in range(2):
            bound = limit(layer, 0, 2 * side - 1)
            for z in range(zc):
                put(z + 1, side * (yc + 1), value(halo.yface[side, z]), bound)
        for zp in range(1, zc + 1):
            tiles(zp, (0, half - 1))
        carry = jnp.zeros((ch, LANES), F32), jnp.zeros((ch, LANES), F32)
        for z in range(1, zc - 1):
            carry = total(z, carry)
        halo.wait(False)
        for side in range(2):
            bound = limit(layer, 2 * side - 1, 0)
            for y in range(yc):
                put(side * (zc + 1), y + 1, value(halo.zface[side, y]), bound)
            for other in range(2):
                bound = limit(layer, 2 * side - 1, 2 * other - 1)
                put(side * (zc + 1), other * (yc + 1), value(halo.corner[side * 2 + other]), bound)
            tiles(side * (zc + 1), range(half))
        for z in (0, zc - 1):
            carry = total(z, carry)
        return carry

    class Stats:
        def __init__(self, phase, rows):
            self.phase, self.count = phase, len(rows)
            for r, row in enumerate(rows):
                stat[phase, me, r : r + 1, :] = row
            for k in far:
                self.copy(k, True).start()

        def copy(self, k, mine):
            at = me if mine else slot_of(k)
            ref = stat.at[self.phase, at, pl.ds(0, self.count)]
            sems = stat_s.at[self.phase, k], stat_r.at[self.phase, at]
            return remote(ref, ref, *sems, member(k))

        def wait(self):
            for k in range(1, group):
                self.copy(k, False).wait_recv()
                self.copy(k, True).wait_send()

        def rows(self, r):
            return [stat[self.phase, i, r : r + 1, :] for i in range(group)]

    def tree(op, parts):
        while len(parts) > 1:
            parts = [op(*parts[i : i + 2]) if i + 1 < len(parts) else parts[i] for i in range(0, len(parts), 2)]
        return parts[0]

    def sums_row(s, q):
        return lane_row(jnp.sum(s, axis=1, keepdims=True), 0) + lane_row(
            jnp.sum(q, axis=1, keepdims=True), HALF
        )

    def norm_of(total, n, start, cells, gain, shift):
        mean = to_column(total, n, start) / cells
        spread = to_column(total, n, start + HALF) / cells - mean * mean
        scaling = lax.rsqrt(spread + norm_eps) * gain
        return mean, scaling, shift

    def act_of(norm, wide=True):
        n = norm[0].shape[0]
        mean, scaling, offset = (
            tuple(jnp.broadcast_to(a, (n, LANES)) for a in norm) if wide else norm
        )

        def act(v, rows=slice(None)):
            normed = (v - mean[rows]) * scaling[rows] + offset[rows]
            return jnp.maximum(normed, leak_slope * normed)

        return act

    def build(dst, taps):
        out = taps.shape[1]
        for a in range(3):
            parts = [taps[9 * a + k].astype(F32) for k in range(9)]
            dst[a * out : (a + 1) * out, :] = jnp.concatenate(parts, axis=1).astype(BF16)

    def plain(v):
        return v.astype(F32)

    build(w1, c1)
    halo0.blank()
    peak0 = fine_inner(vol, plain, 0)
    build(w2, c2)
    build(w3.at[my_y], c3)
    build(w4.at[my_y], c4)
    own_gain = to_column(gc[0:1, :], oc, 0)
    own_shift = to_column(sc[0:1, :], oc, 0)
    grow[my_y, 0:1, :] = lane_row(own_gain, my_y * oc) + lane_row(own_shift, HALF + my_y * oc)
    for halo in (halo1, halo2, halo3):
        halo.blank()
    s, q = fine_conv(w1, halo0, plain, 0, vals1)
    stats = Stats(0, [sums_row(s, q)])
    halo1.start()

    def gathers(mine):
        out = []
        for k in range(1, ny):
            other = ys[k]
            at = my_y if mine else other
            for i, buf in enumerate((grow, w3, w4)):
                out.append(remote(buf.at[at], buf.at[at], w_s.at[i, k], w_r.at[i, at], {"sy": other}))
        return out

    for copy in gathers(True):
        copy.start()
    fine_cells = float(zc * nz * yc * ny * xc)

    def fine_norm(layer):
        total = tree(jnp.add, stats.rows(0))
        gain, shift = to_column(gf[layer : layer + 1, :], ch, 0), to_column(sf[layer : layer + 1, :], ch, 0)
        return norm_of(total, ch, 0, fine_cells, gain, shift)

    stats.wait()
    act = act_of(fine_norm(0))

    peak1 = fine_inner(vals1, act, 1)
    s, q = fine_conv(w2, halo1, act, 1, vals2)
    stats = Stats(1, [sums_row(s, q)])

    pick = jnp.where(iota((2 * LANES, LANES), 0) == 2 * iota((2 * LANES, LANES), 1), 1.0, 0.0).astype(BF16)
    for z in range(hz):
        for t in range(pairs):
            found = []
            for i in range(2):
                y = 4 * t + 2 * i
                block = [vals2[2 * z + a, y + b] for a in range(2) for b in range(2)]
                m = tree(jnp.maximum, block)
                found.append(jnp.maximum(m, pltpu.roll(m, LANES - 1, 1)))
            m = jnp.concatenate(found, axis=1)
            high = rounded(m)
            middle = rounded(m - high)
            low = m - high - middle
            split = jnp.concatenate([high, middle, low], axis=0).astype(BF16)
            r = jnp.dot(split, pick, preferred_element_type=F32)
            pool[z, t] = r[0:ch] + r[ch : 2 * ch] + r[2 * ch : 3 * ch]
    halo2.start()
    for mine, theirs in zip(gathers(True), gathers(False)):
        theirs.wait_recv()
        mine.wait_send()
    stats.wait()
    act_skip = act_of(fine_norm(1))

    def widen(n, zp, load, wide):
        part = 2 * 8
        where = iota((part, LANES), 1)
        column = lax.rem(where, HALF)
        below = where < HALF
        for r in range(0, n, part):
            xs, us = [], []
            for tp in range(pairs + 2):
                v = load(tp, slice(r, r + part))
                left = jnp.where(column == 0, 0.0, pltpu.roll(v, 1, 1))
                right = jnp.where(column == HALF - 1, 0.0, pltpu.roll(v, LANES - 1, 1))
                xs.append((left, v, right))
                us.append([pltpu.roll(x, HALF, 1) for x in xs[-1]])
            for t in range(pairs):
                cols = slice(t * LANES, (t + 1) * LANES)
                for c in range(3):
                    taps = (
                        jnp.where(below, us[t][c], us[t + 1][c]),
                        xs[t + 1][c],
                        jnp.where(below, us[t + 1][c], us[t + 2][c]),
                    )
                    for b, tap in enumerate(taps):
                        base = (3 * b + c) * n + r
                        wide[zp, base : base + part, cols] = tap.astype(BF16)

    def coarse_conv(w, n, halo, act, layer, wide, store):
        top = jnp.zeros((2 * 8, LANES), F32)

        def inner(zp):
            def load(tp, rows):
                nonlocal top
                if tp in (0, pairs + 1):
                    side = int(tp > 0)
                    bound = limit(layer, 0, 2 * side - 1)
                    v = act(halo.yface[side, zp - 1, rows], rows)
                else:
                    bound = bounds[layer]
                    v = act(halo.src[zp - 1, tp - 1, rows], rows)
                    top = jnp.maximum(top, jnp.abs(v))
                return jnp.clip(v, -bound, bound)

            return load

        def outer(side):
            def load(tp, rows):
                if tp in (0, pairs + 1):
                    other = int(tp > 0)
                    bound = limit(layer, 2 * side - 1, 2 * other - 1)
                    v = act(halo.corner[side * 2 + other, rows], rows)
                else:
                    bound = limit(layer, 2 * side - 1, 0)
                    v = act(halo.zface[side, tp - 1, rows], rows)
                return jnp.clip(v, -bound, bound)

            return load

        def plane(zp, load):
            widen(n, zp, load, wide)
            weights = w[...].reshape(3 * wc, 9 * n)
            prod3[zp] = jnp.dot(weights, wide[zp], preferred_element_type=F32)

        halo.wait(True)
        for zp in range(1, hz + 1):
            plane(zp, inner(zp))
        halo.wait(False)
        for side in range(2):
            plane(side * (hz + 1), outer(side))

        parts = []
        for y in range(ny):
            base = 3 * oc * y
            s = q = jnp.zeros((oc, LANES), F32)
            most = least = None
            for z in range(hz):
                for t in range(pairs):
                    cols = slice(t * LANES, (t + 1) * LANES)
                    v = (
                        prod3[z, base : base + oc, cols]
                        + prod3[z + 1, base + oc : base + 2 * oc, cols]
                        + prod3[z + 2, base + 2 * oc : base + 3 * oc, cols]
                    )
                    store(y, z, t, v)
                    s, q = s + v, q + v * v
                    most = v if most is None else jnp.maximum(most, v)
                    least = -v if least is None else jnp.maximum(least, -v)
            parts.append((s, q, most, least))
        joined = [jnp.concatenate(list(p), axis=0) for p in zip(*parts)]
        return joined, jnp.max(rounded(top))

    def store3(y, z, t, v):
        vals3[z, t, y * oc : (y + 1) * oc, :] = v

    def store4(y, z, t, v):
        vals4[y, z, t] = v

    (s, q, most, least), peak2 = coarse_conv(w3, ch, halo2, act_skip, 2, wide3, store3)
    at = iota((1, LANES), 1)
    row = jnp.zeros((1, LANES), F32)
    for i, value in enumerate((peak0, peak1, peak2)):
        row = jnp.where(at == i, value, row)
    ends = lane_row(jnp.max(most, axis=1, keepdims=True), 0) + lane_row(
        jnp.max(least, axis=1, keepdims=True), HALF
    )
    stats = Stats(2, [sums_row(s, q), ends, row])
    halo3.start()

    for z in range(zc):
        for y in range(yc):
            turn[z, pl.ds(y, ch, yc), :] = act_skip(vals2[z, y])
    for z in range(zc):
        skip_out[:, z] = turn[z].reshape(ch, yc, LANES).astype(BF16)

    coarse_cells = float(hz * nz * pairs * ny * LANES)
    gains = tree(jnp.add, [grow[y, 0:1, :] for y in range(ny)])
    stats.wait()
    third = stats
    total = tree(jnp.add, third.rows(0))
    norm3 = norm_of(total, wc, 0, coarse_cells, to_column(gains, wc, 0), to_column(gains, wc, HALF))
    (s, q, _, _), _ = coarse_conv(w4, wc, halo3, act_of(norm3), 3, wide4, store4)
    stats = Stats(3, [sums_row(s, q)])

    def blocks(mine):
        out = []
        for k in range(1, ny):
            other = ys[k]
            at = my_y if mine else other
            out.append(remote(vals4.at[other], fin.at[at], fin_s.at[k], fin_r.at[at], {"sy": other}))
        return out

    for copy in blocks(True):
        copy.start()
    fin[my_y] = vals4[my_y]

    ends = tree(jnp.maximum, third.rows(1))
    act = act_of(norm3, False)
    high, low = act(to_column(ends, wc, 0)), act(-to_column(ends, wc, HALF))
    peak3 = jnp.max(rounded(jnp.maximum(jnp.abs(high), jnp.abs(low))))
    row = jnp.where(at == 3, peak3, tree(jnp.maximum, third.rows(2)))
    peak_all[my_s, 0:1, :] = row

    def across(k, mine):
        other = ahead(my_s, k, ns)
        slot = my_s if mine else other
        ref = peak_all.at[slot, pl.ds(0, 1)]
        return remote(ref, ref, pa_s.at[k], pa_r.at[slot], {"sample": other})

    for k in range(1, ns):
        across(k, True).start()

    own_gain = to_column(gc[1:2, :], oc, 0)
    own_shift = to_column(sc[1:2, :], oc, 0)
    for mine, theirs in zip(blocks(True), blocks(False)):
        theirs.wait_recv()
        mine.wait_send()
    stats.wait()
    total = tree(jnp.add, stats.rows(0))
    act = act_of(norm_of(total, oc, my_y * oc, coarse_cells, own_gain, own_shift))
    for z in range(hz):
        cells = [act(fin[y, z, t]) for y in range(ny) for t in range(pairs)]
        coarse_out[:, z, :] = jnp.concatenate(cells, axis=1).astype(BF16)

    for k in range(1, ns):
        across(k, False).wait_recv()
        across(k, True).wait_send()
    row = tree(jnp.maximum, [peak_all[i, 0:1, :] for i in range(ns)])
    peak_out[...] = row[0, 0 : peak_out.shape[0]]


def per_device(sizes, volume, hist, c1, c2, c3, c4, gf, sf, gc, sc):
    ns, ny, nz = sizes
    _, ch, zc, yc, xc = volume.shape
    oc = c3.shape[1]
    wc = ny * oc
    hz, pairs = zc // 2, yc // 4
    flat = pairs * ny * LANES
    group = ny * nz
    assert xc == LANES and zc % 2 == 0 and yc % 4 == 0 and wc <= HALF

    args = (volume[0], hist, c1, c2, c3, c4, gf, sf, gc, sc)
    args = tuple(pltpu.with_memory_space_constraint(x, pltpu.HBM) for x in args)
    vmem = pl.BlockSpec(memory_space=pltpu.VMEM)
    dma = pltpu.SemaphoreType.DMA

    def faces(planes, rows, n, dtype):
        return [
            pltpu.VMEM((2, rows, n, LANES), dtype),
            pltpu.VMEM((2, planes, n, LANES), dtype),
            pltpu.VMEM((4, n, LANES), dtype),
        ]

    skip, coarse, peaks = pl.pallas_call(
        functools.partial(network, sizes),
        out_shape=(
            jax.ShapeDtypeStruct((ch, zc, yc, xc), BF16),
            jax.ShapeDtypeStruct((oc, hz, flat), BF16),
            jax.ShapeDtypeStruct((4,), F32),
        ),
        in_specs=[pl.BlockSpec(memory_space=IN_SPACE)] * len(args),
        out_specs=(vmem, vmem, vmem),
        scratch_shapes=[
            *[pltpu.VMEM(a.shape, a.dtype) for a in args],
            pltpu.VMEM((3 * ch, 9 * ch), BF16),
            pltpu.VMEM((3 * ch, 9 * ch), BF16),
            pltpu.VMEM((ny, 3 * oc, 9 * ch), BF16),
            pltpu.VMEM((ny, 3 * oc, 9 * wc), BF16),
            pltpu.VMEM((ny, 8, LANES), F32),
            pltpu.VMEM((zc, ch * yc, LANES), F32),
            pltpu.VMEM((zc, yc, ch, LANES), BF16),
            pltpu.VMEM((zc, yc, ch, LANES), F32),
            pltpu.VMEM((zc, yc, ch, LANES), F32),
            pltpu.VMEM((zc + 2, yc + 2, 3 * ch, LANES), BF16),
            pltpu.VMEM((zc + 2, yc // 2, 3 * ch, 2 * LANES), F32),
            pltpu.VMEM((hz, pairs, ch, LANES), F32),
            pltpu.VMEM((hz, pairs, wc, LANES), F32),
            pltpu.VMEM((ny, hz, pairs, oc, LANES), F32),
            pltpu.VMEM((ny, hz, pairs, oc, LANES), F32),
            pltpu.VMEM((hz + 2, 9 * ch, pairs * LANES), BF16),
            pltpu.VMEM((hz + 2, 9 * wc, pairs * LANES), BF16),
            pltpu.VMEM((hz + 2, 3 * wc, pairs * LANES), F32),
            *faces(zc, yc, ch, BF16),
            *faces(zc, yc, ch, F32),
            *faces(hz, pairs, ch, F32),
            *faces(hz, pairs, wc, F32),
            pltpu.VMEM((4, group, 8, LANES), F32),
            pltpu.VMEM((ns, 8, LANES), F32),
            dma((len(args),)),
            dma((4, 8)),
            dma((4, 8)),
            dma((4, group)),
            dma((4, group)),
            dma((3, ny)),
            dma((3, ny)),
            dma((ny,)),
            dma((ny,)),
            dma((ns,)),
            dma((ns,)),
        ],
        compiler_params=pltpu.CompilerParams(
            collective_id=0, has_side_effects=True, vmem_limit_bytes=VMEM_BYTES
        ),
    )(*args)

    def finish(*refs):
        copies = [pltpu.make_async_copy(refs[i], refs[3 + i], refs[6].at[i]) for i in range(3)]
        for copy in copies:
            copy.start()
        for copy in copies:
            copy.wait()

    anywhere = pl.BlockSpec(memory_space=pl.ANY)
    skip, coarse, peaks = pl.pallas_call(
        finish,
        out_shape=tuple(jax.ShapeDtypeStruct(a.shape, a.dtype) for a in (skip, coarse, peaks)),
        in_specs=[anywhere] * 3,
        out_specs=[anywhere] * 3,
        scratch_shapes=[dma((3,))],
        compiler_params=pltpu.CompilerParams(vmem_limit_bytes=FINISH_BYTES),
    )(skip, coarse, peaks)
    return skip[None], coarse[None], peaks


IN_SPACE = pltpu.HBM
VMEM_BYTES = 20 * 1024 * 1024
FINISH_BYTES = 4 * 1024 * 1024


def solution(mesh):
    sizes = (mesh.shape["sample"], mesh.shape["sy"], mesh.shape["sz"])
    return jax.shard_map(
        functools.partial(per_device, sizes),
        mesh=mesh,
        in_specs=(
            P("sample", None, "sz", "sy", None),
            P(),
            P(),
            P(),
            P(None, "sy", None),
            P(None, "sy", None),
            P(),
            P(),
            P(None, "sy"),
            P(None, "sy"),
        ),
        out_specs=(P("sample", None, "sz", "sy", None), P("sample", "sy", "sz", None), P()),
        check_vma=False,
    )
```
